32 devices in a mesh: row: 4 (over x, core), col: 8 (over z, y).
Axes of the slice: x: 2, y: 2, z: 4, core: 2. Of those that a mesh axis runs over, the one named last changes fastest.
Arguments:
- adjacency: bfloat16 [4096, 65536], P('row', 'col'), may hold values from -0.03125 to 0.03125
- tile_mask: int32 [16, 256], P('row', 'col'), may hold values from 0 to 1, as said below
- operand: bfloat16 [65536, 1024], P('col'), may hold values from -6 to 6
- current: bfloat16 [4096, 1024], P('row', 'col'), may hold values from 0 to 1
Outputs:
- reached: bfloat16 [4096, 1024], P('row', 'col')
- progress: float32 [16], P('row')
The draws below stay inside these ranges and needn't reach their ends.
Inputs may be any that keep to these rules, and one draw needn't show every extreme that they name: Split tile_mask into blocks of 4 tile rows by 32 tile columns, aligned to multiples of these. Every block holds at least one nonzero tile, and a block together with the block in the same tile columns whose tile rows start 32 tile rows farther down (upper half of the slab paired with lower half, in order) holds exactly 128 nonzero tiles.
All inputs are finite; a program needn't handle non-finite values.
Results may differ from the reference program's by a relative error of at most 0.0045.
Values may be sent and summed in bfloat16 or wider, within the bound.
A program may use at most 128 MiB of HBM per device.

```python
import jax
import jax.numpy as jnp

TILE = 256
N = 65536
TR_DEV = 4
TR = 16
W = 1024
TILES_DEV = 32


def draw_tile_mask(key, part):
    n_rows = TR // TR_DEV
    n_cols = N // TILE // TILES_DEV
    capacity = TR_DEV * TILES_DEV
    half_rows = n_rows // 2
    lowest = max(1, capacity // 11)
    upper_counts = jax.random.randint(jax.random.fold_in(key, 11), (half_rows, n_cols), lowest, capacity - lowest + 1)
    counts = jnp.concatenate([upper_counts, capacity - upper_counts], axis=0)
    scores = jax.random.randint(jax.random.fold_in(key, 23), (n_rows, n_cols, capacity), 0, 1048576) * capacity
    scores = scores + jnp.arange(capacity, dtype=jnp.int32)[None, None, :]
    ranks = jnp.argsort(jnp.argsort(scores, axis=-1), axis=-1).astype(jnp.int32)
    nonzero = (ranks < counts[:, :, None]).astype(jnp.int32)
    nonzero = nonzero.reshape(n_rows, n_cols, TR_DEV, TILES_DEV).transpose(0, 2, 1, 3)
    return nonzero.reshape(TR, N // TILE)


def steps_of(rng, dims, shards, least, top_value):
    level, own = 1.0, jax.random.fold_in(rng, 6)
    for dim, parts in shards:
        steps = jnp.exp(jax.random.uniform(jax.random.fold_in(own, dim), (parts,), jnp.float32, least / len(shards), top_value / len(shards)))
        level = level * jnp.repeat(steps, dims[dim] // parts).reshape([-1 if axis == dim else 1 for axis in range(len(dims))])
    return level


def scatter_about(rng, dims, scale, limit, cuts=(), held_as=jnp.bfloat16):
    result = scale * jax.random.normal(rng, dims, jnp.float32)
    if cuts:
        result = result * steps_of(rng, dims, cuts, -0.22, 0.18)
    return jnp.clip(result, -limit, limit).astype(held_as)


def setup_inputs(seed: int = 0) -> dict:
    key_list = jax.random.split(jax.random.key(seed), 5)
    return {
        "adjacency": scatter_about(key_list[0], (TR * TILE, N), (N // 2) ** -0.5, 0.03125, ((0, 4), (1, 8))),
        "tile_mask": draw_tile_mask(jax.random.fold_in(key_list[4], 71), 0),
        "operand": scatter_about(key_list[2], (N, W), 1.0, 6.0, ((0, 8),)),
        "current": jnp.clip(1.0 * jax.random.uniform(key_list[3], (TR * TILE, W), jnp.float32) ** steps_of(key_list[3], (TR * TILE, W), ((0, 4), (1, 8)), -0.2, 0.2), 0.0, 1.0).astype(jnp.bfloat16),
    }


def reference(adjacency, tile_mask, operand, current):
    row_count, col_count = adjacency.shape
    tiles_rows = row_count // TILE
    tiles_cols = col_count // TILE
    keep_tile = tile_mask.astype(jnp.bfloat16)[:, None, :, None]
    masked = (adjacency.reshape(tiles_rows, TILE, tiles_cols, TILE) * keep_tile).reshape(row_count, col_count)
    logits = jnp.dot(masked, operand, preferred_element_type=jnp.float32)
    prior_value = current.astype(jnp.float32)
    lifted = (1.0 - prior_value) * jax.nn.sigmoid(logits)
    reached = (prior_value + lifted).astype(jnp.bfloat16)
    window = operand.shape[1]
    row_gain = jnp.sum(lifted.reshape(tiles_rows, TILE * window), axis=1) / (TILE * window)
    progress = jnp.cumsum(row_gain)
    return reached, progress
```

```python
import functools

import jax
import jax.numpy as jnp
from jax import lax
from jax.experimental import pallas as pl
from jax.experimental.pallas import tpu as pltpu
from jax.sharding import PartitionSpec as P

TILE = 256
MESH = pl.DeviceIdType.MESH


def fast_size(n):
    size = 1
    while n % (size * 2) == 0 and (size * 2) ** 2 <= n:
        size *= 2
    return size


def kernel(
    n_row, n_col, mask_ref, adj_hbm, op_hbm, cur_hbm, out_hbm, prog_ref,
    adj, op, cur, res, own, ysend, yrecv, zsend, zrecv, gains,
    adj_sem, op_sem, cur_sem, res_sem, ysend_sem, yrecv_sem, zsend_sem, zrecv_sem, gsend_sem, grecv_sem,
):
    nb = fast_size(n_col)
    na = n_col // nb
    rows, depth = adj.shape
    chunks = rows // TILE
    tiles = depth // TILE
    width = cur.shape[1]
    row, col = lax.axis_index("row"), lax.axis_index("col")
    a, b = col // nb, lax.rem(col, nb)
    me = row * n_col + col
    n_dev = n_row * n_col

    def rows_of(i):
        return pl.ds(i * TILE if isinstance(i, int) else pl.multiple_of(i * TILE, TILE), TILE)

    def load_adj(i):
        return pltpu.make_async_copy(adj_hbm.at[rows_of(i)], adj.at[rows_of(i)], adj_sem.at[i])

    def load_op(d, e):
        block = lax.rem(a + e, na) * nb + lax.rem(b + d, nb)
        return pltpu.make_async_copy(
            op_hbm.at[:, pl.ds(pl.multiple_of(block * width, width), width)],
            op.at[d, :, pl.ds(e * width, width)],
            op_sem.at[d, e],
        )

    order = list(range(1, nb)) + [0]
    load_adj(0).start()
    for d in order:
        for e in range(na):
            load_op(d, e).start()
        if d == order[0]:
            for i in range(1, chunks):
                load_adj(i).start()
    load_cur = pltpu.make_async_copy(cur_hbm, cur, cur_sem)
    load_cur.start()

    barrier = pltpu.get_barrier_semaphore()

    def greet(k, carry):
        to = lax.rem(me + k, n_dev)
        pl.semaphore_signal(barrier, inc=1, device_id=(to // n_col, lax.rem(to, n_col)), device_id_type=MESH)
        return carry

    lax.fori_loop(1, n_dev, greet, 0)

    def y_copy(d, i):
        return pltpu.make_async_remote_copy(
            src_ref=ysend.at[d - 1, i], dst_ref=yrecv.at[d - 1, i],
            send_sem=ysend_sem.at[d - 1, i], recv_sem=yrecv_sem.at[d - 1, i],
            device_id=(row, a * nb + lax.rem(b + d, nb)), device_id_type=MESH,
        )

    def z_copy(e, i):
        return pltpu.make_async_remote_copy(
            src_ref=zsend.at[e - 1, i], dst_ref=zrecv.at[e - 1, i],
            send_sem=zsend_sem.at[e - 1, i], recv_sem=zrecv_sem.at[e - 1, i],
            device_id=(row, lax.rem(a + e, na) * nb + b), device_id_type=MESH,
        )

    def product(i, d):
        parts = []
        for k in range(tiles):
            keep = jnp.full((1, TILE), mask_ref[i, k].astype(jnp.float32)).astype(jnp.bfloat16)
            parts.append(adj[rows_of(i), pl.ds(k * TILE, TILE)] * keep)
        left = jnp.concatenate(parts, axis=1)
        return jnp.dot(left, op[d], preferred_element_type=jnp.float32)

    def send_z(i):
        for d in range(1, nb):
            y_copy(d, i).wait_recv()
        for e in list(range(1, na)) + [0]:
            span = pl.ds(e * width, width)
            total = own[rows_of(i), span]
            for d in range(1, nb):
                total = total + yrecv[d - 1, i, :, span].astype(jnp.float32)
            if e:
                zsend[e - 1, i] = total.astype(jnp.bfloat16)
                z_copy(e, i).start()
            else:
                own[rows_of(i), span] = total

    lane = lax.broadcasted_iota(jnp.int32, (1, 128), 1)

    def finish(i, mine):
        logits = own[rows_of(i), pl.ds(0, width)]
        for e in range(1, na):
            z_copy(e, i).wait_recv()
            logits = logits + zrecv[e - 1, i].astype(jnp.float32)
        prior = cur[rows_of(i)].astype(jnp.float32)
        lifted = (1.0 - prior) * jax.nn.sigmoid(logits)
        res[rows_of(i)] = (prior + lifted).astype(jnp.bfloat16)
        save(i).start()
        return jnp.where(lane == i, jnp.sum(lifted) / (TILE * width * n_col), mine)

    def save(i):
        return pltpu.make_async_copy(res.at[rows_of(i)], out_hbm.at[rows_of(i)], res_sem.at[i])

    def turn(i, carry):
        load_adj(i).wait()
        for d in order:
            @pl.when(i == 0)
            def _():
                for e in range(na):
                    load_op(d, e).wait()

            if d:
                ysend[d - 1, i] = product(i, d).astype(jnp.bfloat16)

                if d == order[0]:
                    @pl.when(i == 0)
                    def _():
                        pl.semaphore_wait(barrier, n_dev - 1)

                y_copy(d, i).start()
            else:
                own[rows_of(i)] = product(i, d)

        @pl.when(i > 0)
        def _():
            send_z(i - 1)

        return carry

    lax.fori_loop(0, chunks, turn, 0)
    load_cur.wait()
    mine = jnp.zeros((1, 128), jnp.float32)
    mine = lax.fori_loop(0, chunks - 1, finish, mine)
    send_z(chunks - 1)
    mine = finish(chunks - 1, mine)
    gains[me] = mine

    def g_copy(k):
        to = lax.rem(me + k, n_dev)
        return pltpu.make_async_remote_copy(
            src_ref=gains.at[me], dst_ref=gains.at[me],
            send_sem=gsend_sem.at[k], recv_sem=grecv_sem.at[k],
            device_id=(to // n_col, lax.rem(to, n_col)), device_id_type=MESH,
        )

    def g_start(k, carry):
        g_copy(k).start()
        return carry

    def g_wait(k, carry):
        g_copy(k).wait_recv()
        return carry

    def g_sent(k, carry):
        g_copy(k).wait_send()
        return carry

    lax.fori_loop(1, n_dev, g_start, 0)
    for i in range(chunks):
        for d in range(1, nb):
            y_copy(d, i).wait_send()
        for e in range(1, na):
            z_copy(e, i).wait_send()
        save(i).wait()
    lax.fori_loop(1, n_dev, g_wait, 0)
    every = gains[:, 0, :]
    device = lax.broadcasted_iota(jnp.int32, (n_dev, 128), 0)
    place = lax.broadcasted_iota(jnp.int32, (n_dev, 128), 1)
    before = device < row * n_col
    same = device < (row + 1) * n_col
    for i in range(chunks):
        counts = jnp.logical_or(before, jnp.logical_and(same, place <= i))
        prog_ref[i] = jnp.sum(jnp.where(counts, every, 0.0))
    lax.fori_loop(1, n_dev, g_sent, 0)


def local(n_row, n_col, adjacency, tile_mask, operand, current):
    rows, depth = adjacency.shape
    width = current.shape[1]
    chunks = rows // TILE
    nb = fast_size(n_col)
    na = n_col // nb
    n_dev = n_row * n_col
    bf, f32, dma = jnp.bfloat16, jnp.float32, pltpu.SemaphoreType.DMA
    return pl.pallas_call(
        functools.partial(kernel, n_row, n_col),
        out_shape=(
            jax.ShapeDtypeStruct((rows, width), bf),
            jax.ShapeDtypeStruct((chunks,), f32),
        ),
        in_specs=[pl.BlockSpec(memory_space=pltpu.SMEM)] + [pl.BlockSpec(memory_space=pl.ANY)] * 3,
        out_specs=(pl.BlockSpec(memory_space=pl.ANY), pl.BlockSpec(memory_space=pltpu.SMEM)),
        scratch_shapes=[
            pltpu.VMEM((rows, depth), bf),
            pltpu.VMEM((nb, depth, na * width), bf),
            pltpu.VMEM((rows, width), bf),
            pltpu.VMEM((rows, width), bf),
            pltpu.VMEM((rows, na * width), f32),
            pltpu.VMEM((nb - 1, chunks, TILE, na * width), bf),
            pltpu.VMEM((nb - 1, chunks, TILE, na * width), bf),
            pltpu.VMEM((na - 1, chunks, TILE, width), bf),
            pltpu.VMEM((na - 1, chunks, TILE, width), bf),
            pltpu.VMEM((n_dev, 1, 128), f32),
            dma((chunks,)), dma((nb, na)), dma, dma((chunks,)),
            dma((nb - 1, chunks)), dma((nb - 1, chunks)),
            dma((na - 1, chunks)), dma((na - 1, chunks)),
            dma((n_dev,)), dma((n_dev,)),
        ],
        compiler_params=pltpu.CompilerParams(
            collective_id=0, has_side_effects=True, vmem_limit_bytes=60 * 1024 * 1024
        ),
        name="reach",
    )(tile_mask, adjacency, operand, current)


def solution(mesh):
    placed = (P("row", "col"), P("row", "col"), P("col", None), P("row", "col"))
    return jax.shard_map(
        functools.partial(local, mesh.shape["row"], mesh.shape["col"]),
        mesh=mesh, in_specs=placed, out_specs=(P("row", "col"), P("row")), check_vma=False,
    )
```
